32 devices in a mesh: seq: 8 (over z, x), vocab: 4 (over y, core).
Axes of the slice: x: 2, y: 2, z: 4, core: 2. Of those that a mesh axis runs over, the one named last changes fastest.
Arguments:
- hidden: bfloat16 [2, 1024, 2048], P(None, 'seq'), may hold values from -6 to 6
- embedded: bfloat16 [2, 1024, 2048], P(None, 'seq'), may hold values from -6 to 6
- targets: int32 [2, 1024], P(None, 'seq'), may hold values from 0 to 51199
- main_mask: int32 [2, 1024], P(None, 'seq'), may hold values 0 or 1
- mtp_mask: int32 [2, 1024], P(None, 'seq'), may hold values from 0 to 1, as said below
- lengths: int32 [2], replicated, may hold values from 256 to 1024, as said below
- head_weight: bfloat16 [2048, 51200], P(None, ('seq', 'vocab')), may hold values from -7.6733202 to 7.6733202
- projection: bfloat16 [4096, 2048], P(None, 'vocab'), may hold values from -0.09375 to 0.09375
- main_gain: float32 [2048], replicated, may hold values from 0.5 to 1.5
- hidden_gain: float32 [2048], replicated, may hold values from 0.5 to 1.5
- embed_gain: float32 [2048], replicated, may hold values from 0.5 to 1.5
- mtp_gain: float32 [2048], replicated, may hold values from 0.5 to 1.5
Outputs:
- main_tokens: float32 [2, 1024], P(None, 'seq')
- mtp_tokens: float32 [2, 1024], P(None, 'seq')
- total_loss: float32 [], replicated
The draws below stay inside these ranges and needn't reach their ends.
Inputs may be any that keep to these rules, and one draw needn't show every extreme that they name: `mtp_mask`: 1 at every position that is a multiple of 128. `lengths`: the first sequence has length 1024.
All inputs are finite; a program needn't handle non-finite values. No bound on the sum of `main_mask` on one device may be relied on, other than what follows from the above.
Results may differ from the reference program's by a relative error of at most 0.0004.
The reference program's roundings to bfloat16 on the way (of `main_rows`, `previous`, `joined`, `mixed` and `mtp_rows`) count: a program that leaves them out, or rounds other values in their place, can miss the bound.
Values may be sent and summed in bfloat16 or wider, within the bound.
No kernel may reach another device: no remote copies, remote signals or barrier semaphores. Data moves between devices by JAX's collectives and lax.ppermute only.
A program may use at most 128 MiB of HBM per device.

```python
import math
import jax
import jax.numpy as jnp
import numpy as np
from jax import lax

D = 2048
VOCAB = 51200
TOK_DEV = 128
MICRO = 2
SEQ = 1024


def draw_head_weight(key, part):
    key_base = jax.random.fold_in(key, 1)
    result_draw = jnp.clip(jax.random.normal(key_base, (D, VOCAB), jnp.float32), -6.0, 6.0) * (3.0 / math.sqrt(D))
    return result_draw.astype(jnp.bfloat16)


def draw_lengths(key, part):
    drawn = jax.random.randint(jax.random.fold_in(key, 11), (MICRO,), SEQ // 4, SEQ + 1).astype(jnp.int32)
    return drawn.at[0].set(SEQ)


def draw_mtp_mask(key, part):
    levels = jax.random.randint(jax.random.fold_in(key, 23), (MICRO, SEQ), 0, 4)
    position = jnp.arange(SEQ, dtype=jnp.int32)[None, :]
    return jnp.where((position % TOK_DEV == 0) | (levels < 3), 1, 0).astype(jnp.int32)


def touch_ends(values, stream_key, smallest, high):
    extent = values.shape
    place = [jax.random.randint(jax.random.fold_in(stream_key, axis), (), 0, extent[axis]) for axis in range(len(extent))]
    values = values.at[tuple(place)].set(smallest)
    longest = extent.index(max(extent))
    place[longest] = (place[longest] + 1) % extent[longest]
    return values.at[tuple(place)].set(high)


def block_levels(key, shape, shards, least, high):
    gain, own = 1.0, jax.random.fold_in(key, 6)
    for axis_at, blocks in shards:
        draws = jnp.exp(jax.random.uniform(jax.random.fold_in(own, axis_at), (blocks,), jnp.float32, least / len(shards), high / len(shards)))
        gain = gain * jnp.repeat(draws, shape[axis_at] // blocks).reshape([-1 if axis == axis_at else 1 for axis in range(len(shape))])
    return gain


def rank_bounds(count, slope):
    weights = [(1 << 20) // math.isqrt(standing ** slope) + 1 for standing in range(1, count + 1)]
    scale = 1 + sum(weights) // (1 << 30)
    return np.cumsum(np.array([max(1, weight // scale) for weight in weights]))


def ranked(key, dims, number_of, lean):
    table = rank_bounds(number_of, lean)
    ticket = jax.random.randint(jax.random.fold_in(key, 1), dims, 0, int(table[number_of - 1]))
    rank = jnp.searchsorted(jnp.asarray(table, jnp.int32), ticket, side="right")
    return jax.random.permutation(jax.random.fold_in(key, 2), number_of)[rank].astype(jnp.int32)


def scatter_about(key, shape, deviation, limit, cuts=(), kind=jnp.bfloat16):
    loudness = block_levels(key, shape, cuts, -0.22, 0.18) if cuts else 1.0
    result = jax.random.normal(key, shape, jnp.float32) * deviation * loudness
    return jnp.minimum(jnp.maximum(result, -limit), limit).astype(kind)


def setup_inputs(seed: int = 0) -> dict:
    streams_of = jax.random.split(jax.random.key(seed), 13)
    hidden = scatter_about(streams_of[0], (MICRO, SEQ, D), 1.0, 6.0, ((1, 8),))
    embedded = scatter_about(streams_of[1], (MICRO, SEQ, D), 1.0, 6.0, ((1, 8),))
    targets = touch_ends(ranked(streams_of[2], (MICRO, SEQ), VOCAB, 2), jax.random.fold_in(streams_of[2], 3), 0, VOCAB - 1).astype(jnp.int32)
    main_mask = touch_ends((jax.random.randint(streams_of[3], (MICRO, SEQ), 0, 4) < 3).astype(jnp.int32), jax.random.fold_in(streams_of[3], 1), 0, 1)
    mtp_mask = draw_mtp_mask(jax.random.fold_in(streams_of[12], 71), 0)
    lengths = draw_lengths(jax.random.fold_in(streams_of[12], 71), 0)
    head_weight = draw_head_weight(jax.random.fold_in(streams_of[12], 71), 0)
    projection = scatter_about(streams_of[7], (2 * D, D), (2 * D) ** -0.5, 0.09375, ((1, 4),))
    main_gain = jnp.clip(1.0 + 0.1 * jax.random.normal(streams_of[8], (D,), jnp.float32), 0.5, 1.5)
    hidden_gain = jnp.clip(1.0 + 0.1 * jax.random.normal(streams_of[9], (D,), jnp.float32), 0.5, 1.5)
    embed_gain = jnp.clip(1.0 + 0.1 * jax.random.normal(streams_of[10], (D,), jnp.float32), 0.5, 1.5)
    mtp_gain = jnp.clip(1.0 + 0.1 * jax.random.normal(streams_of[11], (D,), jnp.float32), 0.5, 1.5)
    return {"hidden": hidden, "embedded": embedded, "targets": targets, "main_mask": main_mask, "mtp_mask": mtp_mask, "lengths": lengths, "head_weight": head_weight, "projection": projection, "main_gain": main_gain, "hidden_gain": hidden_gain, "embed_gain": embed_gain, "mtp_gain": mtp_gain}


EPSILON = 1e-06
MTP_WEIGHT = 0.3

def normalize(values, gain_vec):
    values = values.astype(jnp.float32)
    mean_square = lax.optimization_barrier(jnp.mean(values * values, axis=-1, keepdims=True))
    return values * lax.rsqrt(mean_square + EPSILON) * gain_vec.astype(jnp.float32)

def cross_entropy(all_rows, wanted, head_weight):
    block_size = math.gcd(512, all_rows.shape[0])
    grouped = all_rows.reshape(-1, block_size, all_rows.shape[1])
    grouped_ids = wanted.reshape(-1, block_size)

    def one_block(block_pair):
        block_rows, block_ids = block_pair
        logits = jnp.dot(block_rows, head_weight, preferred_element_type=jnp.float32)
        highest = lax.optimization_barrier(jnp.max(logits, axis=1))
        exp_total = lax.optimization_barrier(jnp.sum(jnp.exp(logits - highest[:, None]), axis=1))
        target_logit = jnp.take_along_axis(logits, block_ids[:, None].astype(jnp.int32), axis=1)[:, 0]
        return highest + jnp.log(exp_total) - target_logit
    return lax.map(one_block, (grouped, grouped_ids)).reshape(-1)

def reference(hidden, embedded, targets, main_mask, mtp_mask, lengths, head_weight, projection, main_gain, hidden_gain, embed_gain, mtp_gain):
    batches, seq_len, model_width = hidden.shape
    positions = jnp.arange(seq_len, dtype=jnp.int32)[None, :]
    length_col = lengths[:, None]
    keep_main = ((main_mask == 1) & (positions + 1 < length_col)).astype(jnp.float32)
    keep_mtp = ((mtp_mask == 1) & (positions >= 1) & (positions + 1 < length_col)).astype(jnp.float32)
    main_rows = normalize(hidden, main_gain).astype(jnp.bfloat16).reshape(-1, model_width)
    previous = jnp.concatenate([jnp.zeros((batches, 1, model_width), hidden.dtype), hidden[:, :-1, :]], axis=1)
    joined = jnp.concatenate([normalize(previous, hidden_gain), normalize(embedded, embed_gain)], axis=2)
    joined = joined.astype(jnp.bfloat16).reshape(-1, 2 * model_width)
    mixed = jnp.dot(joined, projection, preferred_element_type=jnp.float32).astype(jnp.bfloat16)
    mtp_rows = normalize(mixed, mtp_gain).astype(jnp.bfloat16)
    flat_targets = targets.reshape(-1)
    main_losses = cross_entropy(main_rows, flat_targets, head_weight).reshape(batches, seq_len)
    mtp_losses = cross_entropy(mtp_rows, flat_targets, head_weight).reshape(batches, seq_len)
    main_tokens = keep_main * main_losses
    mtp_tokens = keep_mtp * mtp_losses
    total_loss = jnp.sum(main_tokens) / jnp.maximum(jnp.sum(keep_main), 1.0) + MTP_WEIGHT * jnp.sum(mtp_tokens) / jnp.maximum(jnp.sum(keep_mtp), 1.0)
    return (main_tokens, mtp_tokens, total_loss)
```

```python
import functools

import jax
import jax.numpy as jnp
from jax import lax
from jax.experimental import pallas as pl
from jax.experimental.pallas import tpu as pltpu
from jax.sharding import PartitionSpec as P

EPSILON = 1e-06
MTP_WEIGHT = 0.3
LOWEST = -1e30
NOWHERE = -(1 << 30)
META_ROWS = 8
ROW_ALIGN = 16
TILE_MAX = 800
AXES = ("seq", "vocab")


def normalize(values, gain_vec):
    values = values.astype(jnp.float32)
    mean_square = jnp.mean(values * values, axis=-1, keepdims=True)
    return values * lax.rsqrt(mean_square + EPSILON) * gain_vec


def column_tile(cols):
    return max(
        t for t in range(ROW_ALIGN, min(cols, TILE_MAX) + 1, ROW_ALIGN) if cols % t == 0
    )


def ring_order(mesh):
    count = mesh.shape["seq"]
    coords = [getattr(d, "coords", None) for d in mesh.devices[:, 0]]
    across = len({c[0] for c in coords}) if all(c is not None for c in coords) else 2
    if count % across or across < 2 or (count // across) % 2:
        return list(range(count))
    deep = count // across
    walk = [(0, x) for x in range(across)]
    for z in range(1, deep):
        line = list(range(1, across))
        walk += [(z, x) for x in (line[::-1] if z % 2 else line)]
    walk += [(z, 0) for z in range(deep - 1, 0, -1)]
    return [z * across + x for z, x in walk]


def head_kernel(blocks, valid, tile, count, *refs):
    scalars, stats_in, info_in, own, peer = refs[:5]
    sources = refs[5 : 5 + count]
    stats, info, x, wanted, top, total, picked, first, second = refs[5 + count :]
    span = x.shape[0] // len(blocks)
    cols = own.shape[0]
    steps = cols // tile
    stats[...] = stats_in[...]
    info[...] = info_in[...]
    half = stats.shape[1] // 2
    y = scalars[2]
    for at, (head, parts) in enumerate(blocks):
        slot = scalars[3 + at]
        for ref, start, rows, place in parts:
            shift = (0, y * rows, (1 - y) * rows)[place]
            to = pl.multiple_of(at * span + shift, rows)
            x[pl.ds(to, rows), :] = sources[ref][start : start + rows, :]
        if head == 0:
            meta = sources[parts[0][0]][span : span + META_ROWS, :span].astype(jnp.float32)
            ids = meta[0:1] * 256.0 + meta[1:2]
            info[0, pl.ds(slot, 1), :] = ids
            info[0, pl.ds(half + slot, 1), :] = ids
            info[1, pl.ds(slot, 1), :] = meta[2:3]
            info[1, pl.ds(half + slot, 1), :] = meta[3:4]
        ids = info[0, pl.ds(head * half + slot, 1), :].astype(jnp.int32)
        wanted[:, at * span : (at + 1) * span] = jnp.broadcast_to(ids, (8, span))
    top[...] = jnp.full(top.shape, LOWEST, jnp.float32)
    total[...] = jnp.zeros(total.shape, jnp.float32)
    picked[...] = jnp.zeros(picked.shape, jnp.float32)
    second[...] = jnp.full(second.shape, LOWEST, jnp.float32)

    def fold(held, start, base):
        logits = held[...].reshape(tile // 8, 8, x.shape[0])
        place = lax.broadcasted_iota(jnp.int32, logits.shape, 0) * 8
        place += lax.broadcasted_iota(jnp.int32, logits.shape, 1)
        if valid < cols:
            logits = jnp.where(place + start < valid, logits, LOWEST)
        old = top[...]
        new = jnp.maximum(old, jnp.max(logits, axis=0))
        top[...] = new
        fresh = jnp.sum(jnp.exp(logits - new[None]), axis=0)
        total[...] = total[...] * jnp.exp(old - new) + fresh
        hit = place == (wanted[...] - (base + start))[None]
        picked[...] += jnp.sum(jnp.where(hit, logits, 0.0), axis=0)

    def product(weights, start):
        return lax.dot_general(
            weights[pl.ds(start, tile), :],
            x[...],
            (((1,), (1,)), ((), ())),
            preferred_element_type=jnp.float32,
        )

    def step(j, _):
        start = pl.multiple_of(j * tile, tile)
        first[...] = product(own, start)
        fold(second, start - tile, jnp.where(j > 0, scalars[1], NOWHERE))
        second[...] = product(peer, start)
        fold(first, start, scalars[0])
        return 0

    lax.fori_loop(0, steps, step, 0)
    fold(second, cols - tile, scalars[1])
    highest = jnp.max(top[...], axis=0, keepdims=True)
    sums = jnp.sum(total[...] * jnp.exp(top[...] - highest), axis=0, keepdims=True)
    chosen = jnp.sum(picked[...], axis=0, keepdims=True)
    for at, (head, _) in enumerate(blocks):
        lanes = slice(at * span, (at + 1) * span)
        slot = pl.ds(head * half + scalars[3 + at], 1)
        stats[0, slot, :] = highest[:, lanes]
        stats[1, slot, :] = sums[:, lanes]
        stats[2, slot, :] = chosen[:, lanes]


def head_stats(scalars, state, own, peer, valid, sources, blocks):
    cols, width = own.shape
    tile = column_tile(cols)
    span = state[0].shape[2]
    rows = len(blocks) * span
    vmem = pl.BlockSpec(memory_space=pltpu.VMEM)
    wide = pltpu.VMEM((8, rows), jnp.float32)
    return pl.pallas_call(
        functools.partial(head_kernel, blocks, valid, tile, len(sources)),
        in_specs=[pl.BlockSpec(memory_space=pltpu.SMEM)] + [vmem] * (4 + len(sources)),
        out_specs=[vmem, vmem],
        out_shape=[jax.ShapeDtypeStruct(s.shape, s.dtype) for s in state],
        scratch_shapes=[
            pltpu.VMEM((rows, width), jnp.bfloat16),
            pltpu.VMEM((8, rows), jnp.int32),
            wide,
            wide,
            wide,
            pltpu.VMEM((tile, rows), jnp.float32),
            pltpu.VMEM((tile, rows), jnp.float32),
        ],
        compiler_params=pltpu.CompilerParams(vmem_limit_bytes=12 * 1024 * 1024),
        cost_estimate=pl.CostEstimate(
            flops=4 * rows * cols * width,
            bytes_accessed=4 * cols * width + 2 * rows * width,
            transcendentals=2 * rows * cols,
        ),
        name=f"head_{rows}",
    )(scalars, *state, own, peer, *sources)


def join_stats(earlier, latter):
    highest = jnp.maximum(earlier[0], latter[0])
    exp_total = earlier[1] * jnp.exp(earlier[0] - highest)
    exp_total += latter[1] * jnp.exp(latter[0] - highest)
    return jnp.stack([highest, exp_total, earlier[2] + latter[2]])


def ordered(swap, mine, other):
    return jnp.where(swap, other, mine), jnp.where(swap, mine, other)


def shards(
    order,
    hidden,
    embedded,
    targets,
    main_mask,
    mtp_mask,
    lengths,
    head_weight,
    projection,
    main_gain,
    hidden_gain,
    embed_gain,
    mtp_gain,
):
    batches, seq_len, model_width = hidden.shape
    seq_index = lax.axis_index("seq")
    vocab_index = lax.axis_index("vocab")
    seq_count = lax.axis_size("seq")
    vocab_count = lax.axis_size("vocab")
    core = vocab_index & 1
    row = vocab_index >> 1
    block_cols = head_weight.shape[1]
    span = batches * seq_len // 2

    def across(value, mask):
        pairs = [(v, v ^ mask) for v in range(vocab_count)]
        return lax.ppermute(value, "vocab", pairs)

    own = head_weight.T
    padding = -block_cols % ROW_ALIGN
    if padding:
        own = jnp.pad(own, ((0, padding), (0, 0)))
    peer = across(own, 1)

    route = [(i - 1, i) for i in range(1, seq_count)]
    incoming = lax.ppermute(hidden[:, seq_len - 1 :, :], "seq", route)

    positions = seq_index * seq_len + lax.broadcasted_iota(jnp.int32, (batches, seq_len), 1)
    inside = positions + 1 < lengths[:, None]
    keep_main = (main_mask == 1) & inside
    keep_mtp = (mtp_mask == 1) & inside & (positions >= 1)
    fields = jnp.stack(
        [targets // 256, targets % 256, keep_main.astype(jnp.int32), keep_mtp.astype(jnp.int32)]
    )

    def half(value):
        parts = value.reshape((2, span) + value.shape[1:])
        return parts

    flat_hidden = half(hidden.reshape(-1, model_width))
    mine = jnp.where(core == 0, flat_hidden[0], flat_hidden[1])
    main_rows = normalize(mine, main_gain).astype(jnp.bfloat16)
    flat_fields = fields.reshape(4, 2, span)
    meta = jnp.where(core == 0, flat_fields[:, 0], flat_fields[:, 1]).astype(jnp.bfloat16)
    meta = jnp.pad(meta, ((0, META_ROWS - 4), (0, model_width - span)))
    main_block = jnp.concatenate([main_rows, meta], axis=0)

    def flat(s, v):
        return s * vocab_count + v

    following = {s: order[(i + 1) % seq_count] for i, s in enumerate(order)}
    leading = {b: a for a, b in following.items()}
    onward = [
        (flat(s, v), flat((leading if v & 1 else following)[s], v))
        for s in range(seq_count)
        for v in range(vocab_count)
    ]
    backward = [(b, a) for a, b in onward]

    def hops(block, pairs, steps):
        found = []
        for _ in range(steps):
            block = lax.ppermute(block, AXES, pairs)
            found.append(block)
        return found

    far = seq_count // 2
    main_on = hops(main_block, onward, far)
    main_back = hops(main_block, backward, far - 1)

    previous = jnp.concatenate([incoming, hidden[:, : seq_len - 1, :]], axis=1)
    joined = jnp.concatenate(
        [normalize(previous, hidden_gain), normalize(embedded, embed_gain)], axis=2
    )
    joined = joined.astype(jnp.bfloat16).reshape(-1, 2 * model_width)
    partial_value = jnp.dot(joined, projection, preferred_element_type=jnp.float32).astype(
        jnp.bfloat16
    )
    split = vocab_count == 4
    if split:
        halves = half(partial_value)
        kept, sent = ordered(core == 1, halves[0], halves[1])
        pair = jnp.concatenate(ordered(core == 1, kept, across(sent, 1)), axis=1)
        parts = pair.reshape(2, span // 2, pair.shape[1])
        kept, sent = ordered(row == 1, parts[0], parts[1])
        mixed = jnp.concatenate(ordered(row == 1, kept, across(sent, 2)), axis=1)
    else:
        mixed = lax.all_gather(partial_value, "vocab", axis=1, tiled=True)
        mixed = half(mixed)
        mixed = jnp.where(core == 0, mixed[0], mixed[1])
    mtp_block = normalize(mixed, mtp_gain).astype(jnp.bfloat16)
    mtp_on = hops(mtp_block, onward, far - 1)
    mtp_back = hops(mtp_block, backward, far)

    place = jnp.int32(0)
    for i, s in enumerate(order):
        place = jnp.where(seq_index == s, i, place)
    sign = 1 - 2 * core

    def slot(distance):
        return (place - sign * distance) & (seq_count - 1)

    base_own = (seq_index * vocab_count + vocab_index) * block_cols
    base_peer = (seq_index * vocab_count + (vocab_index ^ 1)) * block_cols
    state = [
        jnp.zeros((3, 2 * seq_count, span), jnp.float32),
        jnp.zeros((2, 2 * seq_count, span), jnp.float32),
    ]

    def run(state, items):
        sources, blocks = [], []
        for head, _, parts in items:
            pieces = []
            for array, start, rows, where in parts:
                known = [i for i, s in enumerate(sources) if s is array]
                if not known:
                    sources.append(array)
                    known = [len(sources) - 1]
                pieces.append((known[0], start, rows, where))
            blocks.append((head, tuple(pieces)))
        scalars = jnp.stack([base_own, base_peer, row] + [slot(d) for _, d, _ in items])
        return head_stats(scalars, state, own, peer, block_cols, sources, tuple(blocks))

    def main_item(distance, block):
        return (0, distance, [(block, 0, span, 0)])

    def mtp_items(distances, blocks):
        if not split:
            return [(1, d, [(b, 0, span, 0)]) for d, b in zip(distances, blocks)]
        rows = span // 2
        other = across(jnp.concatenate(blocks) if len(blocks) > 1 else blocks[0], 2)
        return [
            (1, d, [(b, 0, rows, 1), (other, i * rows, rows, 2)])
            for i, (d, b) in enumerate(zip(distances, blocks))
        ]

    for k in range(1, far):
        state = run(state, [main_item(k, main_on[k - 1]), main_item(-k, main_back[k - 1])])
        if k == 1:
            state = run(state, [main_item(0, main_block)] + mtp_items([0], [mtp_block]))
        else:
            state = run(state, mtp_items([k - 1, 1 - k], [mtp_on[k - 2], mtp_back[k - 2]]))
    state = run(state, mtp_items([far - 1, 1 - far], [mtp_on[far - 2], mtp_back[far - 2]]))
    state = run(
        state, [main_item(far, main_on[far - 1])] + mtp_items([-far], [mtp_back[far - 1]])
    )
    stats, info = state

    bits = [("vocab", 2 << b) for b in range((vocab_count // 2).bit_length() - 1)]
    bits += [("seq", 1 << b) for b in range(seq_count.bit_length() - 1)]

    def swapped(value, chosen):
        masks = {"seq": 0, "vocab": 0}
        for axis, mask in chosen:
            masks[axis] ^= mask
        pairs = [
            (flat(s, v), flat(s ^ masks["seq"], v ^ masks["vocab"]))
            for s in range(seq_count)
            for v in range(vocab_count)
        ]
        return lax.ppermute(value, AXES, pairs)

    def is_set(bit):
        return (seq_index if bit[0] == "seq" else vocab_index) & bit[1] != 0

    for at in range(0, len(bits), 2):
        low, high = bits[at], bits[at + 1] if at + 1 < len(bits) else None
        near = swapped(stats, [low])
        if high is None:
            stats = join_stats(*ordered(is_set(low), stats, near))
        else:
            far_low, far_high = swapped(stats, [high]), swapped(stats, [low, high])
            here = ordered(is_set(low), stats, near)
            there = ordered(is_set(low), far_low, far_high)
            (a, c), (b, d) = (
                ordered(is_set(high), here[0], there[0]),
                ordered(is_set(high), here[1], there[1]),
            )
            stats = join_stats(join_stats(a, b), join_stats(c, d))

    losses = stats[0] + jnp.log(stats[1]) - stats[2]
    tokens = (info[1] * losses).reshape(2, seq_count, span)
    keeps = info[1].reshape(2, seq_count, span)
    at_own = jnp.arange(seq_count, dtype=jnp.int32)[:, None] == place
    shown = jnp.sum(jnp.where(at_own, tokens, 0.0), axis=1)
    packed = jnp.concatenate([shown, jnp.sum(tokens, axis=1), jnp.sum(keeps, axis=1)], axis=0)
    packed = jnp.stack(ordered(core == 1, packed, across(packed, 1)))
    main_tokens = packed[:, 0].reshape(batches, seq_len)
    mtp_tokens = packed[:, 1].reshape(batches, seq_len)
    sums = jnp.sum(packed[:, 2:], axis=(0, 2))
    total_loss = sums[0] / jnp.maximum(sums[2], 1.0) + MTP_WEIGHT * sums[1] / jnp.maximum(
        sums[3], 1.0
    )
    return (main_tokens, mtp_tokens, total_loss)


def solution(mesh):
    return jax.shard_map(
        functools.partial(shards, ring_order(mesh)),
        mesh=mesh,
        in_specs=(
            P(None, "seq", None),
            P(None, "seq", None),
            P(None, "seq"),
            P(None, "seq"),
            P(None, "seq"),
            P(),
            P(None, ("seq", "vocab")),
            P(None, "vocab"),
            P(),
            P(),
            P(),
            P(),
        ),
        out_specs=(P(None, "seq"), P(None, "seq"), P()),
        check_vma=False,
    )
```

```python
import functools

import jax
import jax.numpy as jnp
from jax import lax
from jax.experimental import pallas as pl
from jax.experimental.pallas import tpu as pltpu
from jax.sharding import PartitionSpec as P


EPSILON = 1e-06
MTP_WEIGHT = 0.3
LOWEST = -1e30
META_ROWS = 8
ROW_ALIGN = 16
TILE_MAX = 800
VMEM_LIMIT = 4 * 1024 * 1024
VMEM_MOST = 56 * 1024 * 1024
AXES = ("seq", "vocab")


def normalize(values, gain_vec):
    values = values.astype(jnp.float32)
    mean_square = jnp.mean(values * values, axis=-1, keepdims=True)
    return values * lax.rsqrt(mean_square + EPSILON) * gain_vec


def column_tiles(cols):
    tile = max(
        t for t in range(ROW_ALIGN, min(cols, TILE_MAX) + 1, ROW_ALIGN) if cols % t == 0
    )
    even = [(start, tile) for start in range(0, cols, tile)]
    half = tile // 2
    if half % ROW_ALIGN:
        return even, even
    return even, even[:-1] + [(cols - tile, half), (cols - half, half)]


def ring_order(mesh):
    count = mesh.shape["seq"]
    coords = [getattr(d, "coords", None) for d in mesh.devices[:, 0]]
    across = len({c[0] for c in coords}) if all(c is not None for c in coords) else 2
    if count % across or across < 2 or (count // across) % 2:
        return list(range(count))
    deep = count // across
    walk = [(0, x) for x in range(across)]
    for z in range(1, deep):
        line = list(range(1, across))
        walk += [(z, x) for x in (line[::-1] if z % 2 else line)]
    walk += [(z, 0) for z in range(deep - 1, 0, -1)]
    return [z * across + x for z, x in walk]


def head_kernel(segments, valid, count, fetch, *refs):
    scalars, state_in, ids_in, own, peer = refs[:5]
    sources = refs[5 : 5 + count]
    state, ids_out, *rest = refs[5 + count :]
    if fetch:
        held, x, wanted, top, total, picked, first, second, sem = rest
        arrival = pltpu.make_async_copy(peer, held, sem)
        arrival.start()
        peer = held
    else:
        x, wanted, top, total, picked, first, second = rest
    span = x.shape[0] // len(segments)
    cols = own.shape[0]
    state[...] = state_in[...]
    ids_out[...] = ids_in[...]
    half = state.shape[1] // 2
    y, core = scalars[2], scalars[6]

    def slot_of(head, distance, batch):
        block = (scalars[3] - scalars[4] * distance) & (half // 2 - 1)
        return head * half + 2 * block + (core if batch is None else batch)

    for at, (head, distance, batch, meta, parts) in enumerate(segments):
        for ref, start, rows, place in parts:
            shift = (0, y * rows, (1 - y) * rows, 0)[place]
            to = pl.multiple_of(at * span + shift, rows)
            if place == 3:
                start = pl.multiple_of(core * rows, rows)
            x[pl.ds(to, rows), :] = sources[ref][pl.ds(start, rows), :]
        slot = pl.ds(slot_of(head, distance, batch), 1)
        if meta:
            below = slot_of(1, distance, batch)
            ref, start = meta
            fields = sources[ref][start : start + META_ROWS, :span].astype(jnp.float32)
            low, high = fields[:4], fields[4:8]
            if batch is None:
                fields = jnp.where(core == 0, low, high)
            else:
                fields = high if batch else low
            ids = fields[0:1] * 256.0 + fields[1:2]
            ids_out[slot, :] = ids
            ids_out[pl.ds(below, 1), :] = ids
            state[3, slot, :] = fields[2:3]
            state[3, pl.ds(below, 1), :] = fields[3:4]
        ids = ids_out[slot, :].astype(jnp.int32)
        ids = jnp.broadcast_to(ids, (8, span)) - lax.broadcasted_iota(jnp.int32, (8, span), 0)
        wanted[:, at * span : (at + 1) * span] = ids
    top[...] = jnp.full(top.shape, LOWEST, jnp.float32)
    total[...] = jnp.zeros(total.shape, jnp.float32)
    picked[...] = jnp.zeros(picked.shape, jnp.float32)

    def fold(held, start, tile, base):
        logits = held[:tile, :].reshape(tile // 8, 8, x.shape[0])
        if valid < cols:
            place = lax.broadcasted_iota(jnp.int32, logits.shape, 0) * 8
            place += lax.broadcasted_iota(jnp.int32, logits.shape, 1)
            logits = jnp.where(place + start < valid, logits, LOWEST)
        old = top[...]
        new = jnp.maximum(old, jnp.max(logits, axis=0))
        top[...] = new
        offset = wanted[...] - (base + start)
        fresh = total[...] * jnp.exp(old - new)
        chosen = picked[...]
        for i in range(tile // 8):
            fresh += jnp.exp(logits[i] - new)
            reached = offset == 8 * i
            if valid < cols:
                reached &= logits[i] > LOWEST
            chosen = jnp.where(reached, logits[i], chosen)
        total[...] = fresh
        picked[...] = chosen

    waiting = None
    at = 0
    own_tiles, peer_tiles = column_tiles(cols)
    for weights, base, tiles in ((own, scalars[0], own_tiles), (peer, scalars[1], peer_tiles)):
        if fetch and weights is peer:
            arrival.wait()
        for start, tile in tiles:
            space = (first, second)[at % 2]
            space[:tile, :] = lax.dot_general(
                weights[start : start + tile, :],
                x[...],
                (((1,), (1,)), ((), ())),
                preferred_element_type=jnp.float32,
            )
            if waiting:
                fold(*waiting)
            waiting = (space, start, tile, base)
            at += 1
    fold(*waiting)
    highest = jnp.max(top[...], axis=0, keepdims=True)
    sums = jnp.sum(total[...] * jnp.exp(top[...] - highest), axis=0, keepdims=True)
    chosen = jnp.sum(picked[...], axis=0, keepdims=True)
    for at, (head, distance, batch, _, _) in enumerate(segments):
        lanes = slice(at * span, (at + 1) * span)
        slot = pl.ds(slot_of(head, distance, batch), 1)
        state[0, slot, :] = highest[:, lanes]
        state[1, slot, :] = sums[:, lanes]
        state[2, slot, :] = chosen[:, lanes]


def head_stats(scalars, state, own, peer, valid, sources, segments, fetch):
    cols, width = own.shape
    tile = column_tiles(cols)[0][0][1]
    span = state[0].shape[2]
    rows = len(segments) * span
    vmem = pl.BlockSpec(memory_space=pltpu.VMEM)
    wide = pltpu.VMEM((8, rows), jnp.float32)
    spaces = [
        pltpu.VMEM((rows, width), jnp.bfloat16),
        pltpu.VMEM((8, rows), jnp.int32),
        wide,
        wide,
        wide,
        pltpu.VMEM((tile, rows), jnp.float32),
        pltpu.VMEM((tile, rows), jnp.float32),
    ]
    peer_spec = pl.BlockSpec(memory_space=pltpu.HBM) if fetch else vmem
    kept = [*state, peer] if fetch else state
    return pl.pallas_call(
        functools.partial(head_kernel, segments, valid, len(sources), fetch),
        in_specs=[pl.BlockSpec(memory_space=pltpu.SMEM), vmem, vmem, vmem, peer_spec]
        + [vmem] * len(sources),
        out_specs=[vmem] * len(kept),
        out_shape=[jax.ShapeDtypeStruct(s.shape, s.dtype) for s in kept],
        scratch_shapes=spaces + [pltpu.SemaphoreType.DMA] * fetch,
        compiler_params=pltpu.CompilerParams(vmem_limit_bytes=VMEM_LIMIT),
        cost_estimate=pl.CostEstimate(
            flops=4 * rows * cols * width,
            bytes_accessed=4 * cols * width + 2 * rows * width,
            transcendentals=2 * rows * cols,
        ),
    )(scalars, *state, own, peer, *sources)


def normal_rows(values, gain):
    values = values.astype(jnp.float32)
    mean_square = jnp.mean(values * values, axis=-1, keepdims=True)
    return (values * lax.rsqrt(mean_square + EPSILON) * gain).astype(jnp.bfloat16)


def main_kernel(parts, scalars, lengths, hidden, gain, targets, main_mask, mtp_mask, *refs):
    block, rows, gains, ids, mains, mtps, sems = refs
    batches, share, width = rows.shape
    seq_len = share * parts
    y, first_position = scalars[2], scalars[5]
    start = pl.multiple_of(y * share, share) if parts > 1 else 0
    pairs = [(hidden.at[:, pl.ds(start, share)], rows), (gain, gains)]
    pairs += [(targets, ids), (main_mask, mains), (mtp_mask, mtps)]
    copies = [pltpu.make_async_copy(a, b, sems.at[i]) for i, (a, b) in enumerate(pairs)]
    for copy in copies:
        copy.start()
    for copy in copies:
        copy.wait()
    place = lax.broadcasted_iota(jnp.int32, (1, seq_len), 1) + first_position
    fields = []
    for batch in range(batches):
        block[batch * share : (batch + 1) * share, :] = normal_rows(rows[batch], gains[...])
        here = slice(batch, batch + 1)
        inside = place + 1 < lengths[batch]
        keep_main = (mains[here, :] == 1) & inside
        keep_mtp = (mtps[here, :] == 1) & inside & (place >= 1)
        digits = [ids[here, :] >> 8, ids[here, :] & 255]
        fields += [d.astype(jnp.float32) for d in digits]
        fields += [jnp.where(k, 1.0, 0.0) for k in (keep_main, keep_mtp)]
    below = slice(batches * share, batches * share + META_ROWS)
    block[below, :seq_len] = jnp.concatenate(fields, axis=0).astype(jnp.bfloat16)
    block[below, seq_len:] = jnp.zeros((META_ROWS, width - seq_len), jnp.bfloat16)


def main_rows_below(parts, scalars, lengths, hidden, gain, targets, main_mask, mtp_mask):
    batches, seq_len, width = hidden.shape
    smem = pl.BlockSpec(memory_space=pltpu.SMEM)
    far = pl.BlockSpec(memory_space=pltpu.HBM)
    whole = pltpu.VMEM((batches, seq_len), jnp.int32)
    shape = (batches * seq_len // parts + META_ROWS, width)
    return pl.pallas_call(
        functools.partial(main_kernel, parts),
        in_specs=[smem, smem] + [far] * 5,
        out_specs=pl.BlockSpec(memory_space=pltpu.VMEM),
        out_shape=jax.ShapeDtypeStruct(shape, jnp.bfloat16),
        scratch_shapes=[
            pltpu.VMEM((batches, seq_len // parts, width), jnp.bfloat16),
            pltpu.VMEM(gain.shape, jnp.float32),
            whole,
            whole,
            whole,
            pltpu.SemaphoreType.DMA((5,)),
        ],
        compiler_params=pltpu.CompilerParams(vmem_limit_bytes=VMEM_MOST),
        cost_estimate=pl.CostEstimate(
            flops=2 * batches * seq_len * width, bytes_accessed=hidden.size, transcendentals=0
        ),
        name="main_rows",
    )(scalars, lengths, hidden, gain, targets, main_mask, mtp_mask)


def mine_kernel(scalars, hidden, gain, mine):
    mine[...] = normal_rows(hidden[scalars[6]], gain[...])


def main_rows_mine(scalars, hidden, gain):
    vmem = pl.BlockSpec(memory_space=pltpu.VMEM)
    shape = hidden.shape[1:]
    return pl.pallas_call(
        mine_kernel,
        in_specs=[pl.BlockSpec(memory_space=pltpu.SMEM), vmem, vmem],
        out_specs=vmem,
        out_shape=jax.ShapeDtypeStruct(shape, jnp.bfloat16),
        compiler_params=pltpu.CompilerParams(vmem_limit_bytes=VMEM_LIMIT),
        cost_estimate=pl.CostEstimate(
            flops=2 * shape[0] * shape[1], bytes_accessed=hidden.size, transcendentals=0
        ),
        name="mine",
    )(scalars, hidden, gain)


def half_kernel(share, below, scalars, block, half):
    start = pl.multiple_of(scalars[6] * share, share)
    half[:share, :] = block[pl.ds(start, share), :]
    if below:
        half[share:, :] = block[2 * share :, :]


def half_of(scalars, block, share, below):
    vmem = pl.BlockSpec(memory_space=pltpu.VMEM)
    shape = (share + below, block.shape[1])
    return pl.pallas_call(
        functools.partial(half_kernel, share, below),
        in_specs=[pl.BlockSpec(memory_space=pltpu.SMEM), vmem],
        out_specs=vmem,
        out_shape=jax.ShapeDtypeStruct(shape, block.dtype),
        compiler_params=pltpu.CompilerParams(vmem_limit_bytes=VMEM_LIMIT),
        cost_estimate=pl.CostEstimate(
            flops=0, bytes_accessed=4 * shape[0] * shape[1], transcendentals=0
        ),
        name="half",
    )(scalars, block)


def mix_kernel(hidden, incoming, first_gain, embedded, second_gain, projection, out, *held):
    earlier, before, first_scale, tokens, second_scale, weights, joined, sems = held
    batches, seq_len, width = earlier.shape
    pairs = [(hidden, earlier), (incoming, before), (first_gain, first_scale)]
    pairs += [(embedded, tokens), (second_gain, second_scale), (projection, weights)]
    copies = [pltpu.make_async_copy(a, b, sems.at[i]) for i, (a, b) in enumerate(pairs)]
    for copy in copies:
        copy.start()

    def normal(values, gain):
        values = values.astype(jnp.float32)
        mean_square = jnp.mean(values * values, axis=-1, keepdims=True)
        return values * lax.rsqrt(mean_square + EPSILON) * gain

    for copy in copies[:3]:
        copy.wait()
    top = lax.broadcasted_iota(jnp.int32, (seq_len, width), 0) == 0
    for batch in range(batches):
        rows = slice(batch * seq_len, (batch + 1) * seq_len)
        shifted = pltpu.roll(normal(earlier[batch], first_scale[...]), 1, 0)
        shifted = jnp.where(top, normal(before[batch], first_scale[...]), shifted)
        joined[rows, :width] = shifted.astype(jnp.bfloat16)
    copies[3].wait()
    copies[4].wait()
    for batch in range(batches):
        rows = slice(batch * seq_len, (batch + 1) * seq_len)
        joined[rows, width:] = normal(tokens[batch], second_scale[...]).astype(jnp.bfloat16)
    copies[5].wait()
    out[...] = jnp.dot(
        joined[...], weights[...], preferred_element_type=jnp.float32
    ).astype(jnp.bfloat16)


def projected(*operands):
    hidden, projection = operands[0], operands[-1]
    batches, seq_len, width = hidden.shape
    rows, cols = batches * seq_len, projection.shape[1]
    far = pl.BlockSpec(memory_space=pltpu.HBM)
    return pl.pallas_call(
        mix_kernel,
        in_specs=[far] * len(operands),
        out_specs=pl.BlockSpec(memory_space=pltpu.VMEM),
        out_shape=jax.ShapeDtypeStruct((rows, cols), jnp.bfloat16),
        scratch_shapes=[pltpu.VMEM(a.shape, a.dtype) for a in operands]
        + [pltpu.VMEM((rows, 2 * width), jnp.bfloat16), pltpu.SemaphoreType.DMA((6,))],
        compiler_params=pltpu.CompilerParams(vmem_limit_bytes=VMEM_MOST),
        cost_estimate=pl.CostEstimate(
            flops=4 * rows * width * cols, bytes_accessed=2 * projection.size, transcendentals=0
        ),
        name="mix",
    )(*operands)


def arrange_kernel(scalars, mine, beside, above, across, gain, out):
    width = out.shape[1]
    part = width // 4
    y, core = scalars[2], scalars[6]
    quarters = [(mine, y, core), (beside, y, 1 - core)]
    quarters += [(above, 1 - y, core), (across, 1 - y, 1 - core)]
    square = 0.0
    for quarter, _, _ in quarters:
        values = quarter[...].astype(jnp.float32)
        square += jnp.sum(values * values, axis=-1, keepdims=True)
    scale = lax.rsqrt(square / width + EPSILON)
    for quarter, at_y, at_core in quarters:
        lanes = pl.ds(pl.multiple_of((2 * at_y + at_core) * part, part), part)
        values = quarter[...].astype(jnp.float32) * scale * gain[:, lanes]
        out[:, lanes] = values.astype(jnp.bfloat16)


def arranged(scalars, quarters, gain):
    rows, width = quarters[0].shape[0], gain.shape[1]
    vmem = pl.BlockSpec(memory_space=pltpu.VMEM)
    return pl.pallas_call(
        arrange_kernel,
        in_specs=[pl.BlockSpec(memory_space=pltpu.SMEM)] + [vmem] * 5,
        out_specs=vmem,
        out_shape=jax.ShapeDtypeStruct((rows, width), jnp.bfloat16),
        compiler_params=pltpu.CompilerParams(vmem_limit_bytes=VMEM_LIMIT),
        cost_estimate=pl.CostEstimate(
            flops=4 * rows * width, bytes_accessed=4 * rows * width, transcendentals=rows
        ),
        name="arrange",
    )(scalars, *quarters, gain)


def join_stats(earlier, latter):
    highest = jnp.maximum(earlier[0], latter[0])
    exp_total = earlier[1] * jnp.exp(earlier[0] - highest)
    exp_total += latter[1] * jnp.exp(latter[0] - highest)
    return jnp.stack([highest, exp_total, earlier[2] + latter[2]])


def ordered(swap, mine, other):
    return jnp.where(swap, other, mine), jnp.where(swap, mine, other)


def shards(
    order,
    hidden,
    embedded,
    targets,
    main_mask,
    mtp_mask,
    lengths,
    head_weight,
    projection,
    main_gain,
    hidden_gain,
    embed_gain,
    mtp_gain,
):
    batches, seq_len, _ = hidden.shape
    seq_index = lax.axis_index("seq")
    vocab_index = lax.axis_index("vocab")
    seq_count = lax.axis_size("seq")
    vocab_count = lax.axis_size("vocab")
    core = vocab_index & 1
    row = vocab_index >> 1
    block_cols = head_weight.shape[1]
    parts = 2 if vocab_count == 4 else 1
    share = seq_len // parts
    far = seq_count // 2

    def across(value, mask):
        pairs = [(v, v ^ mask) for v in range(vocab_count)]
        return lax.ppermute(value, "vocab", pairs)

    own = head_weight.T
    padding = -block_cols % ROW_ALIGN
    if padding:
        own = jnp.pad(own, ((0, padding), (0, 0)))
    peer = across(own, 1)
    route = [(i - 1, i) for i in range(1, seq_count)]
    incoming = lax.ppermute(hidden[:, seq_len - 1 :, :], "seq", route)

    place = jnp.int32(0)
    for i, s in enumerate(order):
        place = jnp.where(seq_index == s, i, place)
    base_own = (seq_index * vocab_count + vocab_index) * block_cols
    base_peer = (seq_index * vocab_count + (vocab_index ^ 1)) * block_cols
    scalars = jnp.stack(
        [base_own, base_peer, row, place, 1 - 2 * core, seq_index * seq_len, core]
    )

    gain_row = main_gain.reshape(1, -1)
    main_block = main_rows_below(
        parts, scalars, lengths, hidden, gain_row, targets, main_mask, mtp_mask
    )
    main_mine = main_rows_mine(scalars, hidden, gain_row)

    def flat(s, v):
        return s * vocab_count + v

    following = {s: order[(i + 1) % seq_count] for i, s in enumerate(order)}
    leading = {b: a for a, b in following.items()}
    onward = [
        (flat(s, v), flat((leading if v & 1 else following)[s], v))
        for s in range(seq_count)
        for v in range(vocab_count)
    ]

    def hops(block, half):
        found = []
        for at in range(1, far + 1):
            if at == far:
                block = half(block)
            block = lax.ppermute(block, AXES, onward)
            found.append(block)
        return found

    def main_half(block):
        return half_of(scalars, block, share, META_ROWS)

    main_hops = hops(main_block, main_half)
    main_others = [across(block, 2) if parts > 1 else None for block in main_hops]

    partial_value = projected(
        hidden,
        incoming,
        hidden_gain.reshape(1, -1),
        embedded,
        embed_gain.reshape(1, -1),
        projection,
    )
    if parts > 1:
        beside = across(partial_value, 1)
        above = across(partial_value, 2)
        quarters = (partial_value, beside, above, across(above, 1))
        mtp_block = arranged(scalars, quarters, mtp_gain.reshape(1, -1))
    else:
        mixed = lax.all_gather(partial_value, "vocab", axis=1, tiled=True)
        mtp_block = normalize(mixed, mtp_gain).astype(jnp.bfloat16)

    def mtp_half(block):
        return half_of(scalars, block, seq_len, 0)

    mtp_hops = hops(mtp_block, mtp_half)

    slots = 4 * seq_count
    empty = [LOWEST, 0.0, 0.0, 0.0]
    state = [
        jnp.stack([jnp.full((slots, seq_len), e, jnp.float32) for e in empty]),
        jnp.zeros((slots, seq_len), jnp.float32),
    ]
    columns = [own, peer]

    def run(state, segments, fetch=False):
        sources = []

        def number(array):
            known = [i for i, s in enumerate(sources) if s is array]
            if not known:
                sources.append(array)
                known = [len(sources) - 1]
            return known[0]

        known = []
        for head, distance, batch, meta, pieces in segments:
            pieces = tuple((number(p[0]),) + p[1:] for p in pieces)
            meta = (number(meta[0]), meta[1]) if meta else None
            known.append((head, distance, batch, meta, pieces))
        out = head_stats(
            scalars, state, *columns, block_cols, sources, tuple(known), fetch
        )
        if fetch:
            columns[1] = out[2]
        return out[:2]

    def main_segment(at, batch):
        block, other = main_hops[at - 1], main_others[at - 1]
        start = 0 if at == far else batch * share
        pieces = [(block, start, share, 1 if parts > 1 else 0)]
        if parts > 1:
            pieces.append((other, start, share, 2))
        meta = (block, share if at == far else 2 * share)
        return (0, at, batch, meta, pieces)

    def main_pair(at):
        return [main_segment(at, batch) for batch in range(2)]

    def mtp_pair(at):
        meta = (main_hops[at - 1], 2 * share)
        return [
            (1, at, batch, meta, [(mtp_hops[at - 1], batch * seq_len, seq_len, 0)])
            for batch in range(2)
        ]

    own_rows = [
        (0, 0, None, (main_block, 2 * share), [(main_mine, 0, seq_len, 0)]),
        (1, 0, None, None, [(mtp_block, 0, seq_len, 3)]),
    ]
    state = run(state, own_rows, True)
    for at in range(1, far):
        state = run(state, mtp_pair(at))
        state = run(state, main_pair(at))
    last_rows = [
        main_segment(far, None),
        (1, far, None, None, [(mtp_hops[far - 1], 0, seq_len, 0)]),
    ]
    stats, _ = run(state, last_rows)

    bits = [("vocab", 2 << b) for b in range((vocab_count // 2).bit_length() - 1)]
    bits += [("seq", 1 << b) for b in range(seq_count.bit_length() - 1)]

    def swapped(value, chosen):
        masks = {"seq": 0, "vocab": 0}
        for axis, mask in chosen:
            masks[axis] ^= mask
        pairs = [
            (flat(s, v), flat(s ^ masks["seq"], v ^ masks["vocab"]))
            for s in range(seq_count)
            for v in range(vocab_count)
        ]
        return lax.ppermute(value, AXES, pairs)

    def is_set(bit):
        return (seq_index if bit[0] == "seq" else vocab_index) & bit[1] != 0

    stats, others = ordered(core == 1, stats, swapped(stats, [("vocab", 1)]))
    keeps = stats[3] + others[3]
    stats = join_stats(stats, others)
    for at in range(0, len(bits), 2):
        low, high = bits[at], bits[at + 1] if at + 1 < len(bits) else None
        near = swapped(stats, [low])
        if high is None:
            stats = join_stats(*ordered(is_set(low), stats, near))
        else:
            far_low, far_high = swapped(stats, [high]), swapped(stats, [low, high])
            here = ordered(is_set(low), stats, near)
            there = ordered(is_set(low), far_low, far_high)
            (a, c), (b, d) = (
                ordered(is_set(high), here[0], there[0]),
                ordered(is_set(high), here[1], there[1]),
            )
            stats = join_stats(join_stats(a, b), join_stats(c, d))

    losses = stats[0] + jnp.log(stats[1]) - stats[2]
    tokens = (keeps * losses).reshape(2, seq_count, batches, seq_len)
    keeps = keeps.reshape(2, seq_count, batches, seq_len)
    shown = lax.dynamic_index_in_dim(tokens, place, axis=1, keepdims=False)
    sums = jnp.sum(tokens, axis=(1, 2, 3))
    counts = jnp.maximum(jnp.sum(keeps, axis=(1, 2, 3)), 1.0)
    total_loss = sums[0] / counts[0] + MTP_WEIGHT * sums[1] / counts[1]
    return (shown[0], shown[1], total_loss)


def solution(mesh):
    return jax.shard_map(
        functools.partial(shards, ring_order(mesh)),
        mesh=mesh,
        in_specs=(
            P(None, "seq", None),
            P(None, "seq", None),
            P(None, "seq"),
            P(None, "seq"),
            P(None, "seq"),
            P(),
            P(None, ("seq", "vocab")),
            P(None, "vocab"),
            P(),
            P(),
            P(),
            P(),
        ),
        out_specs=(P(None, "seq"), P(None, "seq"), P()),
        check_vma=False,
    )
```

```python
import functools

import jax
import jax.numpy as jnp
from jax import lax
from jax.experimental import pallas as pl
from jax.experimental.pallas import tpu as pltpu
from jax.sharding import PartitionSpec as P


EPSILON = 1e-06
MTP_WEIGHT = 0.3
LOWEST = -1e30
META_ROWS = 8
ROW_ALIGN = 16
TILE_MAX = 800
VMEM_LIMIT = 4 * 1024 * 1024
VMEM_MOST = 56 * 1024 * 1024
AXES = ("seq", "vocab")


def normalize(values, gain_vec):
    values = values.astype(jnp.float32)
    mean_square = jnp.mean(values * values, axis=-1, keepdims=True)
    return values * lax.rsqrt(mean_square + EPSILON) * gain_vec


def column_tiles(cols):
    tile = max(
        t for t in range(ROW_ALIGN, min(cols, TILE_MAX) + 1, ROW_ALIGN) if cols % t == 0
    )
    even = [(start, tile) for start in range(0, cols, tile)]
    half = tile // 2
    if half % ROW_ALIGN:
        return even, even
    return even, even[:-1] + [(cols - tile, half), (cols - half, half)]


def ring_order(mesh):
    count = mesh.shape["seq"]
    coords = [getattr(d, "coords", None) for d in mesh.devices[:, 0]]
    across = len({c[0] for c in coords}) if all(c is not None for c in coords) else 2
    if count % across or across < 2 or (count // across) % 2:
        return list(range(count))
    deep = count // across
    walk = [(0, x) for x in range(across)]
    for z in range(1, deep):
        line = list(range(1, across))
        walk += [(z, x) for x in (line[::-1] if z % 2 else line)]
    walk += [(z, 0) for z in range(deep - 1, 0, -1)]
    return [z * across + x for z, x in walk]


def head_kernel(segments, valid, count, fetch, *refs):
    scalars, state_in, ids_in, own, peer = refs[:5]
    sources = refs[5 : 5 + count]
    state, ids_out, *rest = refs[5 + count :]
    if fetch:
        held, x, wanted, top, total, picked, first, second, sem = rest
        arrival = pltpu.make_async_copy(peer, held, sem)
        arrival.start()
        peer = held
    else:
        x, wanted, top, total, picked, first, second = rest
    span = x.shape[0] // len(segments)
    cols = own.shape[0]
    state[...] = state_in[...]
    ids_out[...] = ids_in[...]
    half = state.shape[1] // 2
    y, core = scalars[2], scalars[6]

    def slot_of(head, distance, batch):
        block = (scalars[3] - scalars[4] * distance) & (half // 2 - 1)
        return head * half + 2 * block + (core if batch is None else batch)

    for at, (head, distance, batch, meta, parts) in enumerate(segments):
        for ref, start, rows, place in parts:
            shift = (0, y * rows, (1 - y) * rows, 0)[place]
            to = pl.multiple_of(at * span + shift, rows)
            if place == 3:
                start = pl.multiple_of(core * rows, rows)
            x[pl.ds(to, rows), :] = sources[ref][pl.ds(start, rows), :]
        slot = pl.ds(slot_of(head, distance, batch), 1)
        if meta:
            below = slot_of(1, distance, batch)
            ref, start = meta
            fields = sources[ref][start : start + META_ROWS, :span].astype(jnp.float32)
            low, high = fields[:4], fields[4:8]
            if batch is None:
                fields = jnp.where(core == 0, low, high)
            else:
                fields = high if batch else low
            ids = fields[0:1] * 256.0 + fields[1:2]
            ids_out[slot, :] = ids
            ids_out[pl.ds(below, 1), :] = ids
            state[2, slot, :] = fields[2:3]
            state[2, pl.ds(below, 1), :] = fields[3:4]
        ids = ids_out[slot, :].astype(jnp.int32)
        ids = jnp.broadcast_to(ids, (8, span)) - lax.broadcasted_iota(jnp.int32, (8, span), 0)
        wanted[:, at * span : (at + 1) * span] = ids
    top[...] = jnp.full(top.shape, LOWEST, jnp.float32)
    total[...] = jnp.zeros(total.shape, jnp.float32)
    picked[...] = jnp.zeros(picked.shape, jnp.float32)

    def fold(held, start, tile, base):
        logits = held[:tile, :].reshape(tile // 8, 8, x.shape[0])
        if valid < cols:
            place = lax.broadcasted_iota(jnp.int32, logits.shape, 0) * 8
            place += lax.broadcasted_iota(jnp.int32, logits.shape, 1)
            logits = jnp.where(place + start < valid, logits, LOWEST)
        old = top[...]
        new = jnp.maximum(old, jnp.max(logits, axis=0))
        top[...] = new
        offset = wanted[...] - (base + start)
        fresh = [total[...] * jnp.exp(old - new)] + [jnp.zeros(old.shape, jnp.float32)] * 3
        chosen = [picked[...]] + [jnp.zeros(old.shape, jnp.float32)] * 3
        for i in range(tile // 8):
            fresh[i % 4] += jnp.exp(logits[i] - new)
            reached = offset == 8 * i
            if valid < cols:
                reached &= logits[i] > LOWEST
            chosen[i % 4] = jnp.where(reached, logits[i], chosen[i % 4])
        total[...] = (fresh[0] + fresh[1]) + (fresh[2] + fresh[3])
        picked[...] = (chosen[0] + chosen[1]) + (chosen[2] + chosen[3])

    waiting = None
    at = 0
    own_tiles, peer_tiles = column_tiles(cols)
    for weights, base, tiles in ((own, scalars[0], own_tiles), (peer, scalars[1], peer_tiles)):
        if fetch and weights is peer:
            arrival.wait()
        for start, tile in tiles:
            space = (first, second)[at % 2]
            space[:tile, :] = lax.dot_general(
                weights[start : start + tile, :],
                x[...],
                (((1,), (1,)), ((), ())),
                preferred_element_type=jnp.float32,
            )
            if waiting:
                fold(*waiting)
            waiting = (space, start, tile, base)
            at += 1
    fold(*waiting)
    highest = jnp.max(top[...], axis=0, keepdims=True)
    sums = jnp.sum(total[...] * jnp.exp(top[...] - highest), axis=0, keepdims=True)
    weight = highest + jnp.log(sums)
    chosen = jnp.sum(picked[...], axis=0, keepdims=True)
    for at, (head, distance, batch, _, _) in enumerate(segments):
        lanes = slice(at * span, (at + 1) * span)
        slot = pl.ds(slot_of(head, distance, batch), 1)
        state[0, slot, :] = weight[:, lanes]
        state[1, slot, :] = chosen[:, lanes]


def head_stats(scalars, state, own, peer, valid, sources, segments, fetch):
    cols, width = own.shape
    tile = column_tiles(cols)[0][0][1]
    span = state[0].shape[2]
    rows = len(segments) * span
    vmem = pl.BlockSpec(memory_space=pltpu.VMEM)
    wide = pltpu.VMEM((8, rows), jnp.float32)
    spaces = [
        pltpu.VMEM((rows, width), jnp.bfloat16),
        pltpu.VMEM((8, rows), jnp.int32),
        wide,
        wide,
        wide,
        pltpu.VMEM((tile, rows), jnp.float32),
        pltpu.VMEM((tile, rows), jnp.float32),
    ]
    peer_spec = pl.BlockSpec(memory_space=pltpu.HBM) if fetch else vmem
    kept = [*state, peer] if fetch else state
    return pl.pallas_call(
        functools.partial(head_kernel, segments, valid, len(sources), fetch),
        in_specs=[pl.BlockSpec(memory_space=pltpu.SMEM), vmem, vmem, vmem, peer_spec]
        + [vmem] * len(sources),
        out_specs=[vmem] * len(kept),
        out_shape=[jax.ShapeDtypeStruct(s.shape, s.dtype) for s in kept],
        scratch_shapes=spaces + [pltpu.SemaphoreType.DMA] * fetch,
        compiler_params=pltpu.CompilerParams(vmem_limit_bytes=VMEM_LIMIT),
        cost_estimate=pl.CostEstimate(
            flops=4 * rows * cols * width,
            bytes_accessed=4 * cols * width + 2 * rows * width,
            transcendentals=2 * rows * cols,
        ),
    )(scalars, *state, own, peer, *sources)


def normal_rows(values, gain):
    values = values.astype(jnp.float32)
    mean_square = jnp.mean(values * values, axis=-1, keepdims=True)
    return (values * lax.rsqrt(mean_square + EPSILON) * gain).astype(jnp.bfloat16)


def main_kernel(parts, scalars, lengths, hidden, gain, targets, main_mask, mtp_mask, *refs):
    block, rows, gains, ids, mains, mtps, sems = refs
    batches, share, width = rows.shape
    seq_len = share * parts
    y, first_position = scalars[2], scalars[5]
    start = pl.multiple_of(y * share, share) if parts > 1 else 0
    pairs = [(hidden.at[:, pl.ds(start, share)], rows), (gain, gains)]
    pairs += [(targets, ids), (main_mask, mains), (mtp_mask, mtps)]
    copies = [pltpu.make_async_copy(a, b, sems.at[i]) for i, (a, b) in enumerate(pairs)]
    for copy in copies:
        copy.start()
    for copy in copies:
        copy.wait()
    place = lax.broadcasted_iota(jnp.int32, (1, seq_len), 1) + first_position
    fields = []
    for batch in range(batches):
        block[batch * share : (batch + 1) * share, :] = normal_rows(rows[batch], gains[...])
        here = slice(batch, batch + 1)
        inside = place + 1 < lengths[batch]
        keep_main = (mains[here, :] == 1) & inside
        keep_mtp = (mtps[here, :] == 1) & inside & (place >= 1)
        digits = [ids[here, :] >> 8, ids[here, :] & 255]
        fields += [d.astype(jnp.float32) for d in digits]
        fields += [jnp.where(k, 1.0, 0.0) for k in (keep_main, keep_mtp)]
    below = slice(batches * share, batches * share + META_ROWS)
    block[below, :seq_len] = jnp.concatenate(fields, axis=0).astype(jnp.bfloat16)
    block[below, seq_len:] = jnp.zeros((META_ROWS, width - seq_len), jnp.bfloat16)


def main_rows_below(parts, scalars, lengths, hidden, gain, targets, main_mask, mtp_mask):
    batches, seq_len, width = hidden.shape
    smem = pl.BlockSpec(memory_space=pltpu.SMEM)
    far = pl.BlockSpec(memory_space=pltpu.HBM)
    whole = pltpu.VMEM((batches, seq_len), jnp.int32)
    shape = (batches * seq_len // parts + META_ROWS, width)
    return pl.pallas_call(
        functools.partial(main_kernel, parts),
        in_specs=[smem, smem] + [far] * 5,
        out_specs=pl.BlockSpec(memory_space=pltpu.VMEM),
        out_shape=jax.ShapeDtypeStruct(shape, jnp.bfloat16),
        scratch_shapes=[
            pltpu.VMEM((batches, seq_len // parts, width), jnp.bfloat16),
            pltpu.VMEM(gain.shape, jnp.float32),
            whole,
            whole,
            whole,
            pltpu.SemaphoreType.DMA((5,)),
        ],
        compiler_params=pltpu.CompilerParams(vmem_limit_bytes=VMEM_MOST),
        cost_estimate=pl.CostEstimate(
            flops=2 * batches * seq_len * width, bytes_accessed=hidden.size, transcendentals=0
        ),
        name="main_rows",
    )(scalars, lengths, hidden, gain, targets, main_mask, mtp_mask)


def mine_kernel(scalars, hidden, gain, block, value, mine, held):
    held[...] = value[...]
    span = hidden.shape[1]
    mine[:span, :] = normal_rows(hidden[scalars[6]], gain[...])
    mine[span:, :] = block[block.shape[0] - META_ROWS :, :]


def main_rows_mine(scalars, hidden, gain, block, value):
    vmem = pl.BlockSpec(memory_space=pltpu.VMEM)
    shape = (hidden.shape[1] + META_ROWS, hidden.shape[2])
    return pl.pallas_call(
        mine_kernel,
        in_specs=[pl.BlockSpec(memory_space=pltpu.SMEM), vmem, vmem, vmem, vmem],
        out_specs=[vmem, vmem],
        out_shape=[jax.ShapeDtypeStruct(s, jnp.bfloat16) for s in (shape, value.shape)],
        compiler_params=pltpu.CompilerParams(vmem_limit_bytes=VMEM_LIMIT),
        cost_estimate=pl.CostEstimate(
            flops=2 * shape[0] * shape[1], bytes_accessed=hidden.size, transcendentals=0
        ),
        name="mine",
    )(scalars, hidden, gain, block, value)


def half_kernel(share, below, scalars, block, half):
    start = pl.multiple_of(scalars[6] * share, share)
    half[:share, :] = block[pl.ds(start, share), :]
    if below:
        half[share:, :] = block[2 * share :, :]


def half_of(scalars, block, share, below):
    vmem = pl.BlockSpec(memory_space=pltpu.VMEM)
    shape = (share + below, block.shape[1])
    return pl.pallas_call(
        functools.partial(half_kernel, share, below),
        in_specs=[pl.BlockSpec(memory_space=pltpu.SMEM), vmem],
        out_specs=vmem,
        out_shape=jax.ShapeDtypeStruct(shape, block.dtype),
        compiler_params=pltpu.CompilerParams(vmem_limit_bytes=VMEM_LIMIT),
        cost_estimate=pl.CostEstimate(
            flops=0, bytes_accessed=4 * shape[0] * shape[1], transcendentals=0
        ),
        name="half",
    )(scalars, block)


def mix_kernel(hidden, incoming, first_gain, embedded, second_gain, projection, out, *held):
    earlier, before, first_scale, tokens, second_scale, weights, joined, sems = held
    batches, seq_len, width = earlier.shape
    pairs = [(hidden, earlier), (incoming, before), (first_gain, first_scale)]
    pairs += [(embedded, tokens), (second_gain, second_scale), (projection, weights)]
    copies = [pltpu.make_async_copy(a, b, sems.at[i]) for i, (a, b) in enumerate(pairs)]
    for copy in copies:
        copy.start()

    def normal(values, gain):
        values = values.astype(jnp.float32)
        mean_square = jnp.mean(values * values, axis=-1, keepdims=True)
        return values * lax.rsqrt(mean_square + EPSILON) * gain

    for copy in copies[:3]:
        copy.wait()
    top = lax.broadcasted_iota(jnp.int32, (seq_len, width), 0) == 0
    for batch in range(batches):
        rows = slice(batch * seq_len, (batch + 1) * seq_len)
        shifted = pltpu.roll(normal(earlier[batch], first_scale[...]), 1, 0)
        shifted = jnp.where(top, normal(before[batch], first_scale[...]), shifted)
        joined[rows, :width] = shifted.astype(jnp.bfloat16)
    copies[3].wait()
    copies[4].wait()
    for batch in range(batches):
        rows = slice(batch * seq_len, (batch + 1) * seq_len)
        joined[rows, width:] = normal(tokens[batch], second_scale[...]).astype(jnp.bfloat16)
    copies[5].wait()
    out[...] = jnp.dot(
        joined[...], weights[...], preferred_element_type=jnp.float32
    ).astype(jnp.bfloat16)


def projected(*operands):
    hidden, projection = operands[0], operands[-1]
    batches, seq_len, width = hidden.shape
    rows, cols = batches * seq_len, projection.shape[1]
    far = pl.BlockSpec(memory_space=pltpu.HBM)
    return pl.pallas_call(
        mix_kernel,
        in_specs=[far] * len(operands),
        out_specs=pl.BlockSpec(memory_space=pltpu.VMEM),
        out_shape=jax.ShapeDtypeStruct((rows, cols), jnp.bfloat16),
        scratch_shapes=[pltpu.VMEM(a.shape, a.dtype) for a in operands]
        + [pltpu.VMEM((rows, 2 * width), jnp.bfloat16), pltpu.SemaphoreType.DMA((6,))],
        compiler_params=pltpu.CompilerParams(vmem_limit_bytes=VMEM_MOST),
        cost_estimate=pl.CostEstimate(
            flops=4 * rows * width * cols, bytes_accessed=2 * projection.size, transcendentals=0
        ),
        name="mix",
    )(*operands)


def arrange_kernel(scalars, mine, beside, above, across, gain, out):
    width = out.shape[1]
    part = width // 4
    y, core = scalars[2], scalars[6]
    quarters = [(mine, y, core), (beside, y, 1 - core)]
    quarters += [(above, 1 - y, core), (across, 1 - y, 1 - core)]
    square = 0.0
    for quarter, _, _ in quarters:
        values = quarter[...].astype(jnp.float32)
        square += jnp.sum(values * values, axis=-1, keepdims=True)
    scale = lax.rsqrt(square / width + EPSILON)
    for quarter, at_y, at_core in quarters:
        lanes = pl.ds(pl.multiple_of((2 * at_y + at_core) * part, part), part)
        values = quarter[...].astype(jnp.float32) * scale * gain[:, lanes]
        out[:, lanes] = values.astype(jnp.bfloat16)


def arranged(scalars, quarters, gain):
    rows, width = quarters[0].shape[0], gain.shape[1]
    vmem = pl.BlockSpec(memory_space=pltpu.VMEM)
    return pl.pallas_call(
        arrange_kernel,
        in_specs=[pl.BlockSpec(memory_space=pltpu.SMEM)] + [vmem] * 5,
        out_specs=vmem,
        out_shape=jax.ShapeDtypeStruct((rows, width), jnp.bfloat16),
        compiler_params=pltpu.CompilerParams(vmem_limit_bytes=VMEM_LIMIT),
        cost_estimate=pl.CostEstimate(
            flops=4 * rows * width, bytes_accessed=4 * rows * width, transcendentals=rows
        ),
        name="arrange",
    )(scalars, *quarters, gain)


def join_stats(parts):
    highest = functools.reduce(jnp.maximum, [p[0] for p in parts])
    total = sum(jnp.exp(p[0] - highest) for p in parts)
    return jnp.stack([highest + jnp.log(total), sum(p[1] for p in parts)])


def last_kernel(scalars, own, near, far_low, far_high, keep, main, mtp, total, tokens):
    low, high = scalars[7] != 0, scalars[8] != 0
    here = ordered(low, own[...], near[...])
    there = ordered(low, far_low[...], far_high[...])
    first = ordered(high, here[0], there[0])
    second = ordered(high, here[1], there[1])
    parts = [first[0], second[0], first[1], second[1]]
    highest = functools.reduce(jnp.maximum, [p[0] for p in parts])
    weight = highest + jnp.log(sum(jnp.exp(p[0] - highest) for p in parts))
    losses = weight - sum(p[1] for p in parts)
    tokens[...] = keep[...] * losses
    half = tokens.shape[0] // 2
    batches = main.shape[0]
    main[...] = tokens[pl.ds(scalars[3] * batches, batches), :]
    mtp[...] = tokens[pl.ds(half + scalars[3] * batches, batches), :]

    def summed(values):
        return jnp.sum(jnp.sum(values, axis=0, keepdims=True), axis=1, keepdims=True)

    means = [
        summed(tokens[at : at + half, :]) / jnp.maximum(summed(keep[at : at + half, :]), 1.0)
        for at in (0, half)
    ]
    total[...] = means[0] + MTP_WEIGHT * means[1]


def last_step(scalars, parts, keep, batches):
    slots, seq_len = keep.shape
    vmem = pl.BlockSpec(memory_space=pltpu.VMEM)
    shapes = [(batches, seq_len), (batches, seq_len), (1, 1)]
    return pl.pallas_call(
        last_kernel,
        in_specs=[pl.BlockSpec(memory_space=pltpu.SMEM)] + [vmem] * 5,
        out_specs=[vmem] * 3,
        out_shape=[jax.ShapeDtypeStruct(s, jnp.float32) for s in shapes],
        scratch_shapes=[pltpu.VMEM(keep.shape, jnp.float32)],
        compiler_params=pltpu.CompilerParams(vmem_limit_bytes=VMEM_LIMIT),
        cost_estimate=pl.CostEstimate(
            flops=30 * slots * seq_len,
            bytes_accessed=36 * slots * seq_len,
            transcendentals=5 * slots * seq_len,
        ),
        name="last",
    )(scalars, *parts, keep)


def ordered(swap, mine, other):
    return jnp.where(swap, other, mine), jnp.where(swap, mine, other)


def shards(
    order,
    hidden,
    embedded,
    targets,
    main_mask,
    mtp_mask,
    lengths,
    head_weight,
    projection,
    main_gain,
    hidden_gain,
    embed_gain,
    mtp_gain,
):
    batches, seq_len, _ = hidden.shape
    seq_index = lax.axis_index("seq")
    vocab_index = lax.axis_index("vocab")
    seq_count = lax.axis_size("seq")
    vocab_count = lax.axis_size("vocab")
    core = vocab_index & 1
    row = vocab_index >> 1
    block_cols = head_weight.shape[1]
    parts = 2 if vocab_count == 4 else 1
    share = seq_len // parts
    far = seq_count // 2

    def across(value, mask):
        pairs = [(v, v ^ mask) for v in range(vocab_count)]
        return lax.ppermute(value, "vocab", pairs)

    own = head_weight.T
    padding = -block_cols % ROW_ALIGN
    if padding:
        own = jnp.pad(own, ((0, padding), (0, 0)))
    peer = across(own, 1)
    route = [(i - 1, i) for i in range(1, seq_count)]
    incoming = lax.ppermute(hidden[:, seq_len - 1 :, :], "seq", route)

    place = jnp.int32(0)
    for i, s in enumerate(order):
        place = jnp.where(seq_index == s, i, place)
    base_own = (seq_index * vocab_count + vocab_index) * block_cols
    base_peer = (seq_index * vocab_count + (vocab_index ^ 1)) * block_cols
    bits = [("vocab", 2 << b) for b in range((vocab_count // 2).bit_length() - 1)]
    bits += [("seq", 1 << b) for b in range(seq_count.bit_length() - 1)]

    def bit_of(bit):
        return (seq_index if bit[0] == "seq" else vocab_index) & bit[1]

    scalars = [base_own, base_peer, row, place, 1 - 2 * core, seq_index * seq_len, core]
    scalars = jnp.stack(scalars + [bit_of(bit) for bit in bits[-2:]])

    gain_row = main_gain.reshape(1, -1)
    main_block = main_rows_below(
        parts, scalars, lengths, hidden, gain_row, targets, main_mask, mtp_mask
    )

    def flat(s, v):
        return s * vocab_count + v

    following = {s: order[(i + 1) % seq_count] for i, s in enumerate(order)}
    leading = {b: a for a, b in following.items()}
    onward = [
        (flat(s, v), flat((leading if v & 1 else following)[s], v))
        for s in range(seq_count)
        for v in range(vocab_count)
    ]

    def hops(block, half):
        found = []
        for at in range(1, far + 1):
            if at == far:
                block = half(block)
            block = lax.ppermute(block, AXES, onward)
            found.append(block)
        return found

    def main_half(block):
        return half_of(scalars, block, share, META_ROWS)

    main_hops = hops(main_block, main_half)
    main_others = [across(block, 2) if parts > 1 else None for block in main_hops]

    partial_value = projected(
        hidden,
        incoming,
        hidden_gain.reshape(1, -1),
        embedded,
        embed_gain.reshape(1, -1),
        projection,
    )
    main_mine, partial_held = main_rows_mine(scalars, hidden, gain_row, main_block, partial_value)
    if parts > 1:
        beside = across(partial_value, 1)
        above = across(partial_value, 2)
        quarters = (partial_held, beside, above, across(above, 1))
        mtp_block = arranged(scalars, quarters, mtp_gain.reshape(1, -1))
    else:
        mixed = lax.all_gather(partial_value, "vocab", axis=1, tiled=True)
        mtp_block = normalize(mixed, mtp_gain).astype(jnp.bfloat16)

    def mtp_half(block):
        return half_of(scalars, block, seq_len, 0)

    mtp_hops = hops(mtp_block, mtp_half)

    slots = 4 * seq_count
    empty = [LOWEST, 0.0, 0.0]
    state = [
        jnp.stack([jnp.full((slots, seq_len), e, jnp.float32) for e in empty]),
        jnp.zeros((slots, seq_len), jnp.float32),
    ]
    columns = [own, peer]

    def run(state, segments, fetch=False):
        sources = []

        def number(array):
            known = [i for i, s in enumerate(sources) if s is array]
            if not known:
                sources.append(array)
                known = [len(sources) - 1]
            return known[0]

        known = []
        for head, distance, batch, meta, pieces in segments:
            pieces = tuple((number(p[0]),) + p[1:] for p in pieces)
            meta = (number(meta[0]), meta[1]) if meta else None
            known.append((head, distance, batch, meta, pieces))
        out = head_stats(
            scalars, state, *columns, block_cols, sources, tuple(known), fetch
        )
        if fetch:
            columns[1] = out[2]
        return out[:2]

    def main_segment(at, batch):
        block, other = main_hops[at - 1], main_others[at - 1]
        start = 0 if at == far else batch * share
        pieces = [(block, start, share, 1 if parts > 1 else 0)]
        if parts > 1:
            pieces.append((other, start, share, 2))
        meta = (block, share if at == far else 2 * share)
        return (0, at, batch, meta, pieces)

    def main_pair(at):
        return [main_segment(at, batch) for batch in range(2)]

    def mtp_pair(at):
        meta = (main_hops[at - 1], 2 * share)
        return [
            (1, at, batch, meta, [(mtp_hops[at - 1], batch * seq_len, seq_len, 0)])
            for batch in range(2)
        ]

    own_rows = [
        (0, 0, None, (main_mine, seq_len), [(main_mine, 0, seq_len, 0)]),
        (1, 0, None, None, [(mtp_block, 0, seq_len, 3)]),
    ]
    state = run(state, own_rows, True)
    for at in range(1, far):
        state = run(state, main_pair(at))
        state = run(state, mtp_pair(at))
    last_rows = [
        main_segment(far, None),
        (1, far, None, None, [(mtp_hops[far - 1], 0, seq_len, 0)]),
    ]
    stats, _ = run(state, last_rows)

    def swapped(value, chosen):
        masks = {"seq": 0, "vocab": 0}
        for axis, mask in chosen:
            masks[axis] ^= mask
        pairs = [
            (flat(s, v), flat(s ^ masks["seq"], v ^ masks["vocab"]))
            for s in range(seq_count)
            for v in range(vocab_count)
        ]
        return lax.ppermute(value, AXES, pairs)

    others = swapped(stats, [("vocab", 1)])
    keeps = stats[2] + others[2]
    stats = jnp.stack([jnp.maximum(stats[0], others[0]), stats[1] + others[1]])
    groups = [bits[:1]] if len(bits) % 2 else []
    groups += [bits[i : i + 2] for i in range(len(bits) % 2, len(bits), 2)]
    for group in groups:
        near = swapped(stats, group[:1])
        if len(group) == 1:
            stats = join_stats(ordered(bit_of(group[0]) != 0, stats, near))
            continue
        low, high = group
        parts = [stats, near, swapped(stats, [high]), swapped(stats, group)]
        if group is groups[-1]:
            main_tokens, mtp_tokens, total = last_step(scalars, parts, keeps, batches)
            return (main_tokens, mtp_tokens, total.reshape(()))
        here = ordered(bit_of(low) != 0, stats, near)
        there = ordered(bit_of(low) != 0, parts[2], parts[3])
        first = ordered(bit_of(high) != 0, here[0], there[0])
        second = ordered(bit_of(high) != 0, here[1], there[1])
        stats = join_stats([first[0], second[0], first[1], second[1]])


def solution(mesh):
    return jax.shard_map(
        functools.partial(shards, ring_order(mesh)),
        mesh=mesh,
        in_specs=(
            P(None, "seq", None),
            P(None, "seq", None),
            P(None, "seq"),
            P(None, "seq"),
            P(None, "seq"),
            P(),
            P(None, ("seq", "vocab")),
            P(None, "vocab"),
            P(),
            P(),
            P(),
            P(),
        ),
        out_specs=(P(None, "seq"), P(None, "seq"), P()),
        check_vma=False,
    )
```
